16 devices in a mesh: dp: 2 (over y, z), ep: 8 (over x, core).
Axes of the slice: x: 4, y: 2, z: 1, core: 2. Of those that a mesh axis runs over, the one named last changes fastest.
The devices are a block of a 4x4x8 slice.
Arguments:
- x_tok: bfloat16 [16, 1024, 2048], P(('dp', 'ep')), parts along dimension 0
- w_query: bfloat16 [2048, 32, 128], P('ep')
- w_key: bfloat16 [2048, 32, 128], P('ep')
- w_value: bfloat16 [2048, 32, 128], P('ep')
- w_out: bfloat16 [4096, 2048], P('ep')
- w_router: float32 [2048, 128], replicated
- w_gate: bfloat16 [128, 2048, 768], P('ep')
- w_up: bfloat16 [128, 2048, 768], P('ep')
- w_down: bfloat16 [128, 768, 2048], P('ep')
- ws_gate: bfloat16 [2048, 768], P('ep')
- ws_up: bfloat16 [2048, 768], P('ep')
- ws_down: bfloat16 [768, 2048], P('ep')
- expert_ids: int32 [16, 1024, 8], P(('dp', 'ep')), parts along dimension 0
Outputs:
- output: bfloat16 [16, 1024, 2048], P(('dp', 'ep')), parts along dimension 0
There are 2 independent parts. The reference program is written for one: setup_inputs(seed, part) draws one part's arguments, and reference() takes and returns one part's arrays. A program takes and returns all parts, laid end to end along the dimension named above; an argument that names none is the same for every part.
All inputs are finite; a program needn't handle non-finite values.
Results may differ from the reference program's by a relative error of at most 0.0127758.
Values are sent between devices in bfloat16 or wider.
A program may use at most 768 MiB of HBM per device.

```python
import jax
import jax.numpy as jnp
import numpy as np
from jax import lax

SEQS_DEV = 1
SEQ = 1024
GROUP = 8
D = 2048
HEADS = 32
HEAD = 128
EXPERTS = 128
TOP = 8
FF = 768
FFS = 768
CAP = 128
NHOT = 16

EPSILON = 1e-6
TOK_DEV = SEQS_DEV * SEQ
TOKENS = GROUP * TOK_DEV
N_SEQS = GROUP * SEQS_DEV
WIDTH = HEADS * HEAD


def rms_norm(values):
    as_f32 = values.astype(jnp.float32)
    return as_f32 * lax.rsqrt(jnp.mean(as_f32 * as_f32, axis=-1, keepdims=True) + EPSILON)


def swiglu_ffn(row_block, gate_w, up_w, down_w):
    gate_act = jnp.dot(row_block, gate_w, preferred_element_type=jnp.float32)
    up_act = jnp.dot(row_block, up_w, preferred_element_type=jnp.float32)
    middle = (jax.nn.silu(gate_act) * up_act).astype(jnp.bfloat16)
    return jnp.dot(middle, down_w, preferred_element_type=jnp.float32).astype(jnp.bfloat16)


def routing_table():
    rest_count = TOK_DEV * TOP - NHOT * CAP
    cold_count = EXPERTS - NHOT
    run_counts = np.concatenate([np.full(NHOT, CAP), rest_count // cold_count + (np.arange(cold_count) < rest_count % cold_count)])
    return jnp.asarray(np.repeat(np.arange(EXPERTS), run_counts), dtype=jnp.int32)


def device_routing(dev_key, run_ids):
    label_key, order_key = jax.random.split(dev_key)
    labels = jax.random.permutation(label_key, EXPERTS)
    shuffle = jax.random.permutation(order_key, TOK_DEV)
    table = labels[run_ids].reshape(TOP, TOK_DEV).T
    return table[shuffle]


def setup_inputs(seed: int = 0, part: int = 0) -> dict:
    root_key = jax.random.key(seed)
    part_key = jax.random.fold_in(root_key, part)
    tok_key, route_key = jax.random.split(part_key)
    weight_keys = jax.random.split(root_key, 10)

    def gauss(key_w, shape_w, scale):
        return (jax.random.normal(key_w, shape_w, jnp.float32) * scale).astype(jnp.bfloat16)

    run_ids = routing_table()

    def draw_device(dev_key):
        return device_routing(dev_key, run_ids)

    dev_keys = jax.random.split(route_key, GROUP)
    expert_ids = jax.vmap(draw_device)(dev_keys).reshape(N_SEQS, SEQ, TOP)
    return {
        'x_tok': jax.random.normal(tok_key, (N_SEQS, SEQ, D), jnp.float32).astype(jnp.bfloat16),
        'w_query': gauss(weight_keys[0], (D, HEADS, HEAD), 2.0 * D ** -0.5),
        'w_key': gauss(weight_keys[1], (D, HEADS, HEAD), D ** -0.5),
        'w_value': gauss(weight_keys[2], (D, HEADS, HEAD), D ** -0.5),
        'w_out': gauss(weight_keys[3], (WIDTH, D), 2.0 * WIDTH ** -0.5),
        'w_router': jax.random.normal(weight_keys[4], (D, EXPERTS), jnp.float32) * D ** -0.5,
        'w_gate': gauss(weight_keys[5], (EXPERTS, D, FF), D ** -0.5),
        'w_up': gauss(weight_keys[6], (EXPERTS, D, FF), D ** -0.5),
        'w_down': gauss(weight_keys[7], (EXPERTS, FF, D), 2.0 * FF ** -0.5),
        'ws_gate': gauss(weight_keys[8], (D, FFS), D ** -0.5),
        'ws_up': gauss(weight_keys[9], (D, FFS), D ** -0.5),
        'ws_down': gauss(jax.random.fold_in(root_key, 11), (FFS, D), FFS ** -0.5),
        'expert_ids': expert_ids,
    }


def reference(x_tok, w_query, w_key, w_value, w_out, w_router, w_gate, w_up, w_down, ws_gate, ws_up, ws_down, expert_ids):
    normed = rms_norm(x_tok).astype(jnp.bfloat16).reshape(TOKENS, D)

    def project(weight):
        return jnp.dot(normed, weight.reshape(D, WIDTH), preferred_element_type=jnp.float32).astype(jnp.bfloat16).reshape(N_SEQS, SEQ, HEADS, HEAD)

    queries = project(w_query)
    keys_all = project(w_key)
    vals_all = project(w_value)
    causal = jnp.arange(SEQ)[:, None] >= jnp.arange(SEQ)[None, :]

    def one_seq(seq_block):
        query_blk, key_blk, value_blk = seq_block
        scores = jnp.einsum('qhe,khe->hqk', query_blk.astype(jnp.float32), key_blk.astype(jnp.float32)) * (HEAD ** -0.5)
        attn_probs = jax.nn.softmax(jnp.where(causal[None], scores, -1e30), axis=-1).astype(jnp.bfloat16)
        return jnp.einsum('hqk,khe->qhe', attn_probs.astype(jnp.float32), value_blk.astype(jnp.float32)).astype(jnp.bfloat16)

    attended = lax.map(one_seq, (queries, keys_all, vals_all))
    attn_out = jnp.dot(attended.reshape(TOKENS, WIDTH), w_out, preferred_element_type=jnp.float32).astype(jnp.bfloat16)
    residual = (x_tok.reshape(TOKENS, D).astype(jnp.float32) + attn_out.astype(jnp.float32)).astype(jnp.bfloat16)

    hidden = rms_norm(residual)
    logits = jnp.dot(hidden, w_router, preferred_element_type=jnp.float32)
    tok_ids = expert_ids.reshape(TOKENS, TOP)
    gate_probs = jax.nn.softmax(jnp.take_along_axis(logits, tok_ids, axis=1), axis=-1)
    moe_in = hidden.astype(jnp.bfloat16)

    flat_ids = tok_ids.reshape(-1)
    n_assign = TOKENS * TOP
    sort_order = jnp.argsort(flat_ids, stable=True)
    expert_counts = jnp.bincount(flat_ids, length=EXPERTS)
    expert_starts = jnp.cumsum(expert_counts) - expert_counts
    slot_count = GROUP * CAP
    flat_gates = gate_probs.reshape(-1)

    def one_expert(running, piece):
        gate_w, up_w, down_w, start_at, count_of = piece
        slot_picks = jnp.minimum(start_at + jnp.arange(slot_count), n_assign - 1)
        assign_ids = sort_order[slot_picks]
        slot_gate = jnp.where(jnp.arange(slot_count) < count_of, flat_gates[assign_ids], 0.0)
        slot_token = assign_ids // TOP
        outputs = swiglu_ffn(moe_in[slot_token], gate_w, up_w, down_w)
        running = running.at[slot_token].add(slot_gate[:, None] * outputs.astype(jnp.float32))
        return running, None

    routed, unused = lax.scan(one_expert, jnp.zeros((TOKENS, D), jnp.float32), (w_gate, w_up, w_down, expert_starts, expert_counts))
    shared = swiglu_ffn(moe_in, ws_gate, ws_up, ws_down)
    y_out = (residual.astype(jnp.float32) + routed + shared.astype(jnp.float32)).astype(jnp.bfloat16)
    return y_out.reshape(N_SEQS, SEQ, D)
```

```python
import functools
import jax
import jax.numpy as jnp
from jax import lax
from jax.experimental import pallas as pl
from jax.experimental.pallas import tpu as pltpu
from jax.sharding import PartitionSpec as P

EPSILON = 1e-6
HALVES = 2
PARTS = 2
CHUNKS = HALVES * PARTS
ROW_TILE = 192
LANES = 128
SUBLANES = 8
VMEM_BYTES = 66_000_000


def rms_norm(values):
    as_f32 = values.astype(jnp.float32)
    return as_f32 * lax.rsqrt(jnp.mean(as_f32 * as_f32, axis=-1, keepdims=True) + EPSILON)


def expert_kernel(count_ref, token_ref, gate_ref, u_hbm, gate_w, up_w, down_w, out_hbm, u_rows, acc, x_tiles, x_rows, middle, y_tiles, in_sem, out_sem):
    part, expert = pl.program_id(0), pl.program_id(1)
    n_local = pl.num_programs(1)
    group, unused, lane_blocks, unused = u_hbm.shape
    n_tok = u_rows.shape[0] - 1
    per_dev = n_tok // group
    dev_rows = per_dev * lane_blocks
    ff = gate_w.shape[2]
    d_model = gate_w.shape[1]
    row_tile = x_rows.shape[0]

    @pl.when(expert == 0)
    def _():
        loads = []
        for g in range(group):
            source = u_hbm.at[g, pl.ds(pl.multiple_of(part * per_dev, per_dev), per_dev)]
            loads.append(pltpu.make_async_copy(source, u_rows.at[pl.ds(g * per_dev, per_dev)], in_sem.at[g]))
            loads[-1].start()

        def clear(step, carry):
            acc[pl.ds(pl.multiple_of(step * 256, 256), 256), :] = jnp.zeros((256, LANES), jnp.float32)
            return carry

        lax.fori_loop(0, n_tok * lane_blocks // 256, clear, 0)
        for load in loads:
            load.wait()

    count = count_ref[part * n_local + expert]

    def one_tile(tile, carry):
        base = tile * row_tile
        live = jnp.minimum(count - base, row_tile)

        def gather(step, inner):
            for i in range(16):
                token = token_ref[0, 0, 0, base + step * 16 + i]
                group = step * 2 + i // SUBLANES
                start = group * (SUBLANES * lane_blocks) + i % SUBLANES
                x_tiles[pl.ds(start, lane_blocks, stride=SUBLANES), :] = u_rows[token].astype(jnp.float32)
            return inner

        steps = (live + 15) // 16
        lax.fori_loop(0, steps, gather, 0)

        def pack(step, inner):
            span = 2 * SUBLANES * lane_blocks
            tiles = x_tiles[pl.ds(pl.multiple_of(step * span, span), span), :].reshape(2, lane_blocks, SUBLANES, LANES)
            for c in range(lane_blocks):
                pair = jnp.concatenate([tiles[0, c], tiles[1, c]], axis=0).astype(jnp.bfloat16)
                x_rows[pl.ds(pl.multiple_of(step * 16, 16), 16), c * LANES:(c + 1) * LANES] = pair
            return inner

        lax.fori_loop(0, steps, pack, 0)

        for start in range(0, ff, 256):
            cols = slice(start, start + 256)
            gate_act = jnp.dot(x_rows[...], gate_w[0, :, cols], preferred_element_type=jnp.float32)
            up_act = jnp.dot(x_rows[...], up_w[0, :, cols], preferred_element_type=jnp.float32)
            middle[:, cols] = (jax.nn.silu(gate_act) * up_act).astype(jnp.bfloat16)
        for start in range(0, d_model, 256):
            rows_out = jnp.dot(middle[...], down_w[0, :, start:start + 256], preferred_element_type=jnp.float32)
            rows_out = rows_out.astype(jnp.bfloat16).astype(jnp.float32)
            for c in range(256 // LANES):
                for b in range(row_tile // SUBLANES):
                    at = (b * lane_blocks + start // LANES + c) * SUBLANES
                    y_tiles[at:at + SUBLANES, :] = rows_out[b * SUBLANES:(b + 1) * SUBLANES, c * LANES:(c + 1) * LANES]

        def combine(step, inner):
            places, sums = [], []
            for i in range(SUBLANES):
                token = token_ref[0, 0, 0, base + step * SUBLANES + i]
                weight = gate_ref[0, 0, 0, token]
                start = step * (SUBLANES * lane_blocks) + i
                row = y_tiles[pl.ds(start, lane_blocks, stride=SUBLANES), :]
                place = pl.ds(pl.multiple_of(token * lane_blocks, lane_blocks), lane_blocks)
                places.append(place)
                sums.append(acc[place, :] + weight * row)
            for place, total in zip(places, sums):
                acc[place, :] = total
            return inner

        lax.fori_loop(0, (live + SUBLANES - 1) // SUBLANES, combine, 0)
        return carry

    lax.fori_loop(0, (count + row_tile - 1) // row_tile, one_tile, 0)

    @pl.when(expert == n_local - 1)
    def _():
        stores = []
        for g in range(group):
            target = out_hbm.at[g, pl.ds(pl.multiple_of(part * dev_rows, dev_rows), dev_rows)]
            stores.append(pltpu.make_async_copy(acc.at[pl.ds(g * dev_rows, dev_rows)], target, out_sem.at[g]))
            stores[-1].start()
        for store in stores:
            store.wait()


def expert_partials(counts, token_lists, gate_table, u_all, gate_loc, up_loc, down_loc):
    group, held, lane_blocks, unused = u_all.shape
    n_local, d_model, ff = gate_loc.shape
    n_parts, unused, unused, list_len = token_lists.shape
    table_len = gate_table.shape[3]
    n_tok = group * held // n_parts
    rows = n_tok * lane_blocks
    grid_spec = pltpu.PrefetchScalarGridSpec(
        num_scalar_prefetch=1,
        grid=(n_parts, n_local),
        in_specs=[
            pl.BlockSpec((1, 1, 1, list_len), lambda p, e, c: (p, e, 0, 0), memory_space=pltpu.SMEM),
            pl.BlockSpec((1, 1, 1, table_len), lambda p, e, c: (p, e, 0, 0), memory_space=pltpu.SMEM),
            pl.BlockSpec(memory_space=pl.ANY),
            pl.BlockSpec((1, d_model, ff), lambda p, e, c: (e, 0, 0)),
            pl.BlockSpec((1, d_model, ff), lambda p, e, c: (e, 0, 0)),
            pl.BlockSpec((1, ff, d_model), lambda p, e, c: (e, 0, 0)),
        ],
        out_specs=pl.BlockSpec(memory_space=pl.ANY),
        scratch_shapes=[
            pltpu.VMEM((n_tok + 1, lane_blocks, LANES), jnp.bfloat16),
            pltpu.VMEM((rows + lane_blocks, LANES), jnp.float32),
            pltpu.VMEM((ROW_TILE * lane_blocks, LANES), jnp.float32),
            pltpu.VMEM((ROW_TILE, d_model), jnp.bfloat16),
            pltpu.VMEM((ROW_TILE, ff), jnp.bfloat16),
            pltpu.VMEM((ROW_TILE * lane_blocks, LANES), jnp.float32),
            pltpu.SemaphoreType.DMA((group,)),
            pltpu.SemaphoreType.DMA((group,)),
        ],
    )
    flops = 6 * n_parts * n_tok * d_model * ff
    return pl.pallas_call(
        expert_kernel,
        grid_spec=grid_spec,
        out_shape=jax.ShapeDtypeStruct((group, held * lane_blocks, LANES), jnp.float32),
        compiler_params=pltpu.CompilerParams(dimension_semantics=('arbitrary', 'arbitrary'), vmem_limit_bytes=VMEM_BYTES),
        cost_estimate=pl.CostEstimate(flops=flops, bytes_accessed=n_parts * (3 * n_local * d_model * ff * 2 + rows * LANES * 6), transcendentals=0),
        name='routed_experts',
    )(counts, token_lists, gate_table, u_all, gate_loc, up_loc, down_loc)


def local_layer(x_loc, q_shard, k_shard, v_shard, o_shard, w_router, gate_loc, up_loc, down_loc, sgate_shard, sup_shard, sdown_shard, ids_loc, group):
    n_seq, seq_len, d_model = x_loc.shape
    n_heads, head_dim = q_shard.shape[1:]
    n_tok = n_seq * seq_len
    top_k = ids_loc.shape[-1]
    n_local = gate_loc.shape[0]
    n_experts = n_local * group
    lane_blocks = d_model // LANES
    per_chunk = n_tok // CHUNKS
    chunk_tok = group * per_chunk
    per_half = n_tok // HALVES
    first_expert = lax.axis_index('ep') * n_local

    query_w = lax.all_gather(q_shard, 'ep', axis=0, tiled=True)
    key_w = lax.all_gather(k_shard, 'ep', axis=0, tiled=True)
    value_w = lax.all_gather(v_shard, 'ep', axis=0, tiled=True)
    out_w = lax.all_gather(o_shard, 'ep', axis=0, tiled=True)

    ids_t = ids_loc.reshape(n_tok, top_k).T
    ids_all = lax.all_gather(ids_t, 'ep', axis=0)
    local_ids = jnp.arange(n_local, dtype=jnp.int32)[:, None, None, None] + first_expert
    chosen = ids_all[None] == local_ids
    member = jnp.any(chosen, axis=2).reshape(n_local, group, CHUNKS, per_chunk).transpose(2, 0, 1, 3).reshape(CHUNKS, n_local, chunk_tok)
    counts = jnp.sum(member.astype(jnp.int32), axis=-1)
    token_lists = lax.sort(jnp.where(member, jnp.arange(chunk_tok, dtype=jnp.int32), chunk_tok), dimension=2, is_stable=False)

    normed = rms_norm(x_loc).astype(jnp.bfloat16)
    queries = jnp.einsum('bsd,dhe->bshe', normed, query_w, preferred_element_type=jnp.float32).astype(jnp.bfloat16)
    normed_k, token_lists, counts = lax.optimization_barrier((normed, token_lists, counts))
    keys_all = jnp.einsum('bsd,dhe->bshe', normed_k, key_w, preferred_element_type=jnp.float32).astype(jnp.bfloat16)
    scores = jnp.einsum('bqhe,bkhe->bhqk', queries, keys_all, preferred_element_type=jnp.float32) * (head_dim ** -0.5)
    causal = jnp.arange(seq_len)[:, None] >= jnp.arange(seq_len)[None, :]
    attn_probs = jax.nn.softmax(jnp.where(causal, scores, -1e30), axis=-1).astype(jnp.bfloat16)
    normed_v, attn_probs = lax.optimization_barrier((normed, attn_probs))
    vals_all = jnp.einsum('bsd,dhe->bshe', normed_v, value_w, preferred_element_type=jnp.float32).astype(jnp.bfloat16)
    attended = jnp.einsum('bhqk,bkhe->bqhe', attn_probs, vals_all, preferred_element_type=jnp.float32).astype(jnp.bfloat16)
    attended = attended.reshape(n_tok, n_heads * head_dim)
    x_flat = x_loc.reshape(n_tok, d_model)

    residuals, inputs, u_alls, gates = [], [], [], []
    tok_ids = ids_loc.reshape(n_tok, top_k)
    for half in range(HALVES):
        rows = slice(half * per_half, (half + 1) * per_half)
        attn_out = jnp.dot(attended[rows], out_w, preferred_element_type=jnp.float32).astype(jnp.bfloat16)
        residual = (x_flat[rows].astype(jnp.float32) + attn_out.astype(jnp.float32)).astype(jnp.bfloat16)
        residual = lax.optimization_barrier(residual)
        hidden = rms_norm(residual)
        moe_in = hidden.astype(jnp.bfloat16)
        sent, attended = lax.optimization_barrier((moe_in.reshape(per_half, lane_blocks, LANES), attended))
        u_alls.append(lax.all_gather(sent, 'ep', axis=0))
        logits = jnp.dot(hidden, w_router, precision=lax.Precision.HIGHEST, preferred_element_type=jnp.float32)
        hit = tok_ids[rows][:, :, None] == jnp.arange(n_experts, dtype=jnp.int32)
        picked = jnp.sum(jnp.where(hit, logits[:, None, :], 0.0), axis=-1)
        gates.append(jax.nn.softmax(picked, axis=-1))
        residuals.append(residual)
        inputs.append(moe_in)

    gates_t = jnp.concatenate(gates, axis=0).T
    gates_all = lax.all_gather(gates_t, 'ep', axis=0)
    gate_table = jnp.sum(jnp.where(chosen, gates_all[None], 0.0), axis=2)
    gate_table = gate_table.reshape(n_local, group, CHUNKS, per_chunk).transpose(2, 0, 1, 3).reshape(CHUNKS, n_local, 1, chunk_tok)
    gate_table = jnp.pad(gate_table, ((0, 0), (0, 0), (0, 0), (0, LANES)))

    ff_rows, ff_shared = sgate_shard.shape
    shards = jnp.concatenate([sgate_shard, sup_shard, sdown_shard.reshape(-1, ff_shared)], axis=0)
    shards, moe_in = lax.optimization_barrier((shards, jnp.concatenate(inputs, axis=0)))
    shared_all = lax.all_gather(shards, 'ep', axis=0)
    shared_gate = shared_all[:, :ff_rows].reshape(-1, ff_shared)
    shared_up = shared_all[:, ff_rows:2 * ff_rows].reshape(-1, ff_shared)
    shared_down = shared_all[:, 2 * ff_rows:].reshape(-1, d_model)

    gate_act = jnp.dot(moe_in, shared_gate, preferred_element_type=jnp.float32)
    up_act = jnp.dot(moe_in, shared_up, preferred_element_type=jnp.float32)
    shared = jnp.dot((jax.nn.silu(gate_act) * up_act).astype(jnp.bfloat16), shared_down, preferred_element_type=jnp.float32).astype(jnp.bfloat16)

    outs = []
    for half in range(HALVES):
        parts = slice(half * PARTS, (half + 1) * PARTS)
        rows = slice(half * per_half, (half + 1) * per_half)
        partial = expert_partials(counts[parts].reshape(-1), token_lists[parts][:, :, None, :], gate_table[parts], u_alls[half], gate_loc, up_loc, down_loc)
        routed = lax.psum_scatter(partial.reshape(-1, LANES), 'ep', scatter_dimension=0, tiled=True).reshape(per_half, d_model)
        outs.append((residuals[half].astype(jnp.float32) + routed + shared[rows].astype(jnp.float32)).astype(jnp.bfloat16))
    return jnp.concatenate(outs, axis=0).reshape(n_seq, seq_len, d_model)


def solution(mesh):
    tok_spec = P(('dp', 'ep'), None, None)
    row_spec = P('ep', None)
    cube_spec = P('ep', None, None)
    in_specs = (tok_spec, cube_spec, cube_spec, cube_spec, row_spec, P(None, None), cube_spec, cube_spec, cube_spec, row_spec, row_spec, row_spec, tok_spec)
    return jax.shard_map(functools.partial(local_layer, group=mesh.shape['ep']), mesh=mesh, in_specs=in_specs, out_specs=tok_spec, check_vma=False)
```

```python
import functools
import jax
import jax.numpy as jnp
from jax import lax
from jax.experimental import pallas as pl
from jax.experimental.pallas import tpu as pltpu
from jax.sharding import PartitionSpec as P

EPSILON = 1e-6
HALVES = 2
PARTS = 2
CHUNKS = HALVES * PARTS
ROW_TILE = 192
LANES = 128
SUBLANES = 8
VMEM_BYTES = 66_000_000


def rms_norm(values):
    as_f32 = values.astype(jnp.float32)
    return as_f32 * lax.rsqrt(jnp.mean(as_f32 * as_f32, axis=-1, keepdims=True) + EPSILON)


def expert_kernel(first_part, count_ref, token_ref, gate_ref, u_hbm, gate_w, up_w, down_w, out_hbm, u_rows, acc, x_tiles, x_rows, middle, y_tiles, in_sem, out_sem):
    part, expert = pl.program_id(0), pl.program_id(1)
    n_local = pl.num_programs(1)
    group, unused, lane_blocks, unused = u_hbm.shape
    n_tok = u_rows.shape[0] - 1
    per_dev = n_tok // group
    dev_rows = per_dev * lane_blocks
    ff = gate_w.shape[2]
    d_model = gate_w.shape[1]
    row_tile = x_rows.shape[0]

    @pl.when(expert == 0)
    def _():
        loads = []
        for g in range(group):
            source = u_hbm.at[g, pl.ds(pl.multiple_of((first_part + part) * per_dev, per_dev), per_dev)]
            loads.append(pltpu.make_async_copy(source, u_rows.at[pl.ds(g * per_dev, per_dev)], in_sem.at[g]))
            loads[-1].start()

        def clear(step, carry):
            acc[pl.ds(pl.multiple_of(step * 256, 256), 256), :] = jnp.zeros((256, LANES), jnp.float32)
            return carry

        lax.fori_loop(0, n_tok * lane_blocks // 256, clear, 0)
        for load in loads:
            load.wait()

    count = count_ref[part * n_local + expert]

    def one_tile(tile, carry):
        base = tile * row_tile
        live = jnp.minimum(count - base, row_tile)

        def gather(step, inner):
            for i in range(16):
                token = token_ref[0, 0, 0, base + step * 16 + i]
                group = step * 2 + i // SUBLANES
                start = group * (SUBLANES * lane_blocks) + i % SUBLANES
                x_tiles[pl.ds(start, lane_blocks, stride=SUBLANES), :] = u_rows[token].astype(jnp.float32)
            return inner

        steps = (live + 15) // 16
        lax.fori_loop(0, steps, gather, 0)

        def pack(step, inner):
            span = 2 * SUBLANES * lane_blocks
            tiles = x_tiles[pl.ds(pl.multiple_of(step * span, span), span), :].reshape(2, lane_blocks, SUBLANES, LANES)
            for c in range(lane_blocks):
                pair = jnp.concatenate([tiles[0, c], tiles[1, c]], axis=0).astype(jnp.bfloat16)
                x_rows[pl.ds(pl.multiple_of(step * 16, 16), 16), c * LANES:(c + 1) * LANES] = pair
            return inner

        lax.fori_loop(0, steps, pack, 0)

        for start in range(0, ff, 256):
            cols = slice(start, start + 256)
            gate_act = jnp.dot(x_rows[...], gate_w[0, :, cols], preferred_element_type=jnp.float32)
            up_act = jnp.dot(x_rows[...], up_w[0, :, cols], preferred_element_type=jnp.float32)
            middle[:, cols] = (jax.nn.silu(gate_act) * up_act).astype(jnp.bfloat16)
        for start in range(0, d_model, 256):
            rows_out = jnp.dot(middle[...], down_w[0, :, start:start + 256], preferred_element_type=jnp.float32)
            rows_out = rows_out.astype(jnp.bfloat16).astype(jnp.float32)
            for c in range(256 // LANES):
                for b in range(row_tile // SUBLANES):
                    at = (b * lane_blocks + start // LANES + c) * SUBLANES
                    y_tiles[at:at + SUBLANES, :] = rows_out[b * SUBLANES:(b + 1) * SUBLANES, c * LANES:(c + 1) * LANES]

        def combine(step, inner):
            places, sums = [], []
            for i in range(SUBLANES):
                token = token_ref[0, 0, 0, base + step * SUBLANES + i]
                weight = gate_ref[0, 0, 0, token]
                start = step * (SUBLANES * lane_blocks) + i
                row = y_tiles[pl.ds(start, lane_blocks, stride=SUBLANES), :]
                place = pl.ds(pl.multiple_of(token * lane_blocks, lane_blocks), lane_blocks)
                places.append(place)
                sums.append(acc[place, :] + weight * row)
            for place, total in zip(places, sums):
                acc[place, :] = total
            return inner

        lax.fori_loop(0, (live + SUBLANES - 1) // SUBLANES, combine, 0)
        return carry

    lax.fori_loop(0, (count + row_tile - 1) // row_tile, one_tile, 0)

    @pl.when(expert == n_local - 1)
    def _():
        stores = []
        for g in range(group):
            target = out_hbm.at[g, pl.ds(pl.multiple_of(part * dev_rows, dev_rows), dev_rows)]
            stores.append(pltpu.make_async_copy(acc.at[pl.ds(g * dev_rows, dev_rows)], target, out_sem.at[g]))
            stores[-1].start()
        for store in stores:
            store.wait()


def expert_partials(counts, token_lists, gate_table, u_all, gate_loc, up_loc, down_loc, first_part):
    group, held, lane_blocks, unused = u_all.shape
    n_local, d_model, ff = gate_loc.shape
    n_parts, unused, unused, list_len = token_lists.shape
    table_len = gate_table.shape[3]
    n_tok = list_len
    rows = n_tok * lane_blocks
    grid_spec = pltpu.PrefetchScalarGridSpec(
        num_scalar_prefetch=1,
        grid=(n_parts, n_local),
        in_specs=[
            pl.BlockSpec((1, 1, 1, list_len), lambda p, e, c: (p, e, 0, 0), memory_space=pltpu.SMEM),
            pl.BlockSpec((1, 1, 1, table_len), lambda p, e, c: (p, e, 0, 0), memory_space=pltpu.SMEM),
            pl.BlockSpec(memory_space=pl.ANY),
            pl.BlockSpec((1, d_model, ff), lambda p, e, c: (e, 0, 0)),
            pl.BlockSpec((1, d_model, ff), lambda p, e, c: (e, 0, 0)),
            pl.BlockSpec((1, ff, d_model), lambda p, e, c: (e, 0, 0)),
        ],
        out_specs=pl.BlockSpec(memory_space=pl.ANY),
        scratch_shapes=[
            pltpu.VMEM((n_tok + 1, lane_blocks, LANES), jnp.bfloat16),
            pltpu.VMEM((rows + lane_blocks, LANES), jnp.float32),
            pltpu.VMEM((ROW_TILE * lane_blocks, LANES), jnp.float32),
            pltpu.VMEM((ROW_TILE, d_model), jnp.bfloat16),
            pltpu.VMEM((ROW_TILE, ff), jnp.bfloat16),
            pltpu.VMEM((ROW_TILE * lane_blocks, LANES), jnp.float32),
            pltpu.SemaphoreType.DMA((group,)),
            pltpu.SemaphoreType.DMA((group,)),
        ],
    )
    flops = 6 * n_parts * n_tok * d_model * ff
    return pl.pallas_call(
        functools.partial(expert_kernel, first_part),
        grid_spec=grid_spec,
        out_shape=jax.ShapeDtypeStruct((group, n_parts * rows // group, LANES), jnp.float32),
        compiler_params=pltpu.CompilerParams(dimension_semantics=('arbitrary', 'arbitrary'), vmem_limit_bytes=VMEM_BYTES),
        cost_estimate=pl.CostEstimate(flops=flops, bytes_accessed=n_parts * (3 * n_local * d_model * ff * 2 + rows * LANES * 6), transcendentals=0),
        name='routed_experts',
    )(counts, token_lists, gate_table, u_all, gate_loc, up_loc, down_loc)


def local_layer(x_loc, q_shard, k_shard, v_shard, o_shard, w_router, gate_loc, up_loc, down_loc, sgate_shard, sup_shard, sdown_shard, ids_loc, group):
    n_seq, seq_len, d_model = x_loc.shape
    n_heads, head_dim = q_shard.shape[1:]
    n_tok = n_seq * seq_len
    top_k = ids_loc.shape[-1]
    n_local = gate_loc.shape[0]
    n_experts = n_local * group
    lane_blocks = d_model // LANES
    per_chunk = n_tok // CHUNKS
    chunk_tok = group * per_chunk
    per_half = n_tok // HALVES
    first_expert = lax.axis_index('ep') * n_local

    query_w = lax.all_gather(q_shard, 'ep', axis=0, tiled=True)
    key_w = lax.all_gather(k_shard, 'ep', axis=0, tiled=True)
    value_w = lax.all_gather(v_shard, 'ep', axis=0, tiled=True)
    out_w = lax.all_gather(o_shard, 'ep', axis=0, tiled=True)

    ids_t = ids_loc.reshape(n_tok, top_k).T
    ids_all = lax.all_gather(ids_t, 'ep', axis=0)
    local_ids = jnp.arange(n_local, dtype=jnp.int32)[:, None, None, None] + first_expert
    chosen = ids_all[None] == local_ids
    member = jnp.any(chosen, axis=2).reshape(n_local, group, CHUNKS, per_chunk).transpose(2, 0, 1, 3).reshape(CHUNKS, n_local, chunk_tok)
    counts = jnp.sum(member.astype(jnp.int32), axis=-1)
    token_lists = lax.sort(jnp.where(member, jnp.arange(chunk_tok, dtype=jnp.int32), chunk_tok), dimension=2, is_stable=False)

    normed = rms_norm(x_loc).astype(jnp.bfloat16)
    queries = jnp.einsum('bsd,dhe->bshe', normed, query_w, preferred_element_type=jnp.float32).astype(jnp.bfloat16)
    normed_k, token_lists, counts = lax.optimization_barrier((normed, token_lists, counts))
    keys_all = jnp.einsum('bsd,dhe->bshe', normed_k, key_w, preferred_element_type=jnp.float32).astype(jnp.bfloat16)
    scores = jnp.einsum('bqhe,bkhe->bhqk', queries, keys_all, preferred_element_type=jnp.float32) * (head_dim ** -0.5)
    causal = jnp.arange(seq_len)[:, None] >= jnp.arange(seq_len)[None, :]
    attn_probs = jax.nn.softmax(jnp.where(causal, scores, -1e30), axis=-1).astype(jnp.bfloat16)
    normed_v, attn_probs = lax.optimization_barrier((normed, attn_probs))
    vals_all = jnp.einsum('bsd,dhe->bshe', normed_v, value_w, preferred_element_type=jnp.float32).astype(jnp.bfloat16)
    ff_rows, ff_shared = sgate_shard.shape
    shards = jnp.concatenate([sgate_shard, sup_shard, sdown_shard.reshape(-1, ff_shared)], axis=0)
    shards, vals_all = lax.optimization_barrier((shards, vals_all))
    shared_all = lax.all_gather(shards, 'ep', axis=0)
    attended = jnp.einsum('bhqk,bkhe->bqhe', attn_probs, vals_all, preferred_element_type=jnp.float32).astype(jnp.bfloat16)
    attended = attended.reshape(n_tok, n_heads * head_dim)
    x_flat = x_loc.reshape(n_tok, d_model)

    residuals, inputs, u_alls, gates = [], [], [], []
    tok_ids = ids_loc.reshape(n_tok, top_k)
    for half in range(HALVES):
        rows = slice(half * per_half, (half + 1) * per_half)
        attn_out = jnp.dot(attended[rows], out_w, preferred_element_type=jnp.float32).astype(jnp.bfloat16)
        residual = (x_flat[rows].astype(jnp.float32) + attn_out.astype(jnp.float32)).astype(jnp.bfloat16)
        residual = lax.optimization_barrier(residual)
        hidden = rms_norm(residual)
        moe_in = hidden.astype(jnp.bfloat16)
        sent, attended = lax.optimization_barrier((moe_in.reshape(per_half, lane_blocks, LANES), attended))
        if half == 0:
            sent, shared_all = lax.optimization_barrier((sent, shared_all))
        u_alls.append(lax.all_gather(sent, 'ep', axis=0))
        logits = jnp.dot(hidden, w_router, precision=lax.Precision.HIGHEST, preferred_element_type=jnp.float32)
        hit = tok_ids[rows][:, :, None] == jnp.arange(n_experts, dtype=jnp.int32)
        picked = jnp.sum(jnp.where(hit, logits[:, None, :], 0.0), axis=-1)
        gates.append(jax.nn.softmax(picked, axis=-1))
        residuals.append(residual)
        inputs.append(moe_in)

    gates_t = jnp.concatenate(gates, axis=0).T
    gates_all = lax.all_gather(gates_t, 'ep', axis=0)
    gate_table = jnp.sum(jnp.where(chosen, gates_all[None], 0.0), axis=2)
    gate_table = gate_table.reshape(n_local, group, CHUNKS, per_chunk).transpose(2, 0, 1, 3).reshape(CHUNKS, n_local, 1, chunk_tok)
    gate_table = jnp.pad(gate_table, ((0, 0), (0, 0), (0, 0), (0, LANES)))

    moe_in = jnp.concatenate(inputs, axis=0)
    shared_gate = shared_all[:, :ff_rows].reshape(-1, ff_shared)
    shared_up = shared_all[:, ff_rows:2 * ff_rows].reshape(-1, ff_shared)
    shared_down = shared_all[:, 2 * ff_rows:].reshape(-1, d_model)

    gate_act = jnp.dot(moe_in, shared_gate, preferred_element_type=jnp.float32)
    up_act = jnp.dot(moe_in, shared_up, preferred_element_type=jnp.float32)
    shared = jnp.dot((jax.nn.silu(gate_act) * up_act).astype(jnp.bfloat16), shared_down, preferred_element_type=jnp.float32).astype(jnp.bfloat16)

    outs = []
    for first, count in ((0, 1), (1, 1), (2, 2)):
        parts = slice(first, first + count)
        half, first_part = first // PARTS, first % PARTS
        in_half = slice(first_part * per_chunk, (first_part + count) * per_chunk)
        rows = slice(first * per_chunk, (first + count) * per_chunk)
        partial = expert_partials(counts[parts].reshape(-1), token_lists[parts][:, :, None, :], gate_table[parts], u_alls[half], gate_loc, up_loc, down_loc, first_part)
        routed = lax.psum_scatter(partial.reshape(-1, LANES), 'ep', scatter_dimension=0, tiled=True).reshape(count * per_chunk, d_model)
        outs.append((residuals[half][in_half].astype(jnp.float32) + routed + shared[rows].astype(jnp.float32)).astype(jnp.bfloat16))
    return jnp.concatenate(outs, axis=0).reshape(n_seq, seq_len, d_model)


def solution(mesh):
    tok_spec = P(('dp', 'ep'), None, None)
    row_spec = P('ep', None)
    cube_spec = P('ep', None, None)
    in_specs = (tok_spec, cube_spec, cube_spec, cube_spec, row_spec, P(None, None), cube_spec, cube_spec, cube_spec, row_spec, row_spec, row_spec, tok_spec)
    return jax.shard_map(functools.partial(local_layer, group=mesh.shape['ep']), mesh=mesh, in_specs=in_specs, out_specs=tok_spec, check_vma=False)
```
